32 devices in a mesh: ctx: 16 (over z, y, core), head: 2 (over x).
Axes of the slice: x: 2, y: 2, z: 4, core: 2. Of those that a mesh axis runs over, the one named last changes fastest.
Arguments:
- queries: bfloat16 [1792, 16384], P('ctx', 'head'), may hold values from -120 to 120
- keys: bfloat16 [1792, 1024], P('ctx', 'head'), may hold values from -4.5 to 4.5
- values: bfloat16 [1792, 1024], P('ctx', 'head'), may hold values from -6 to 6
- span_pos: int32 [32], replicated, may hold values from 0 to 31, as said below
Outputs:
- attended: bfloat16 [1792, 16384], P(('ctx', 'head'))
The draws below stay inside these ranges and needn't reach their ends.
Inputs may be any that keep to these rules, and one draw needn't show every extreme that they name: `span_pos`: a permutation of 0 to 31; entries 2b and 2b + 1 sum to 31.
All inputs are finite; a program needn't handle non-finite values.
Results may differ from the reference program's by a relative error of at most 0.0049.
Values may be sent and summed in bfloat16 or wider, within the bound.
A program may use at most 64 MiB of HBM per device.

```python
import jax
import jax.numpy as jnp
from jax import lax

HEADS = 128
KV_HEADS = 8
HEAD_DIM = 128
SPAN = 56
TOKENS = 1792
N_CTX = 16


def shared_keys(key):
    base = jax.random.normal(jax.random.fold_in(key, 11), (TOKENS, KV_HEADS, HEAD_DIM), jnp.float32)
    base = jnp.clip(base, -4.5, 4.5)
    return base


def draw_keys(key, part):
    return shared_keys(key).reshape(TOKENS, KV_HEADS * HEAD_DIM).astype(jnp.bfloat16)


def draw_queries(key, part):
    group = HEADS // KV_HEADS
    drawn = jax.random.normal(jax.random.fold_in(key, 21), (TOKENS, KV_HEADS, group, HEAD_DIM), jnp.float32)
    drawn = jnp.clip(drawn, -4.5, 4.5)
    return drawn.reshape(TOKENS, HEADS * HEAD_DIM).astype(jnp.bfloat16)


def draw_span_pos(key, part):
    pairs = TOKENS // (2 * SPAN)
    order = jax.random.permutation(jax.random.fold_in(key, 31), pairs).astype(jnp.int32)
    flips = jax.random.randint(jax.random.fold_in(key, 32), (pairs,), 0, 2)
    later = 2 * pairs - 1 - order
    first = jnp.where(flips == 1, later, order)
    second = jnp.where(flips == 1, order, later)
    return jnp.stack([first, second], axis=1).reshape(-1).astype(jnp.int32)


def levels(stream_key, shape, pieces, smallest, top_value):
    loudness = 1.0
    for dim, blocks in pieces:
        steps = jax.random.uniform(jax.random.fold_in(jax.random.fold_in(stream_key, 6), dim), (blocks,), jnp.float32, smallest / len(pieces), top_value / len(pieces))
        loudness = loudness * jnp.repeat(jnp.exp(steps), shape[dim] // blocks).reshape((-1,) + (1,) * (len(shape) - 1 - dim))
    return loudness


def normal_values(own_key, dims, spread, bound, cuts=(), kind=jnp.bfloat16):
    loudness = levels(own_key, dims, cuts, -0.22, 0.18) if cuts else 1.0
    values = jax.random.normal(own_key, dims, jnp.float32) * spread * loudness
    return jnp.minimum(jnp.maximum(values, -bound), bound).astype(kind)


def setup_inputs(seed: int = 0) -> dict:
    seeds = jax.random.split(jax.random.key(seed), 5)
    return {
        "queries": draw_queries(jax.random.fold_in(seeds[4], 71), 0),
        "keys": draw_keys(jax.random.fold_in(seeds[4], 71), 0),
        "values": normal_values(seeds[2], (TOKENS, KV_HEADS * HEAD_DIM), 1.0, 6.0, ((0, 16), (1, 2))),
        "span_pos": draw_span_pos(jax.random.fold_in(seeds[4], 71), 0),
    }


NEG_FLOOR = -1.0e30


def block_partial(query_block, query_pos, key_block, value_block, key_pos):
    scale = query_block.shape[-1] ** -0.5
    scores = jnp.einsum("qgjd,kgd->gjqk", query_block.astype(jnp.float32), key_block.astype(jnp.float32)) * scale
    visible = key_pos[None, :] <= query_pos[:, None]
    row_max = jnp.max(jnp.where(visible, scores, NEG_FLOOR), axis=-1)
    weights = jnp.where(visible, jnp.exp(scores - row_max[..., None]), 0.0)
    totals = jnp.sum(weights, axis=-1)
    rounded = lax.optimization_barrier(weights.astype(jnp.bfloat16))
    product = jnp.einsum("gjqk,kgd->qgjd", rounded.astype(jnp.float32), value_block.astype(jnp.float32))
    totals_rows = jnp.transpose(totals, (2, 0, 1))
    max_rows = jnp.transpose(row_max, (2, 0, 1))
    seen = totals_rows > 0.0
    safe_totals = jnp.where(seen, totals_rows, 1.0)
    partial_value = jnp.where(seen[..., None], product / safe_totals[..., None], 0.0).astype(jnp.bfloat16)
    log_total = jnp.where(seen, max_rows + jnp.log(safe_totals), NEG_FLOOR)
    return partial_value, log_total


def reference(queries, keys, values, span_pos):
    block_len = 2 * SPAN
    group = HEADS // KV_HEADS
    offsets = jnp.arange(SPAN, dtype=jnp.int32)
    positions = (span_pos.astype(jnp.int32)[:, None] * SPAN + offsets[None, :]).reshape(-1)
    all_pos = positions.reshape(N_CTX, block_len)
    all_queries = queries.reshape(N_CTX, block_len, KV_HEADS, group, HEAD_DIM)
    all_keys = keys.reshape(N_CTX, block_len, KV_HEADS, HEAD_DIM)
    all_values = values.reshape(N_CTX, block_len, KV_HEADS, HEAD_DIM)

    def one_block(inputs):
        query_block, query_pos = inputs

        def step_over(carry, key_inputs):
            top, numer, denom = carry
            key_block, value_block, key_pos = key_inputs
            partial_value, log_total = block_partial(query_block, query_pos, key_block, value_block, key_pos)
            new_top = jnp.maximum(top, log_total)
            older = jnp.exp(top - new_top)
            fresh = jnp.where(log_total > -1.0e29, jnp.exp(log_total - new_top), 0.0)
            numer = numer * older[..., None] + fresh[..., None] * partial_value.astype(jnp.float32)
            denom = denom * older + fresh
            return (new_top, numer, denom), None

        start = (jnp.full((block_len, KV_HEADS, group), NEG_FLOOR, jnp.float32),
                 jnp.zeros((block_len, KV_HEADS, group, HEAD_DIM), jnp.float32),
                 jnp.zeros((block_len, KV_HEADS, group), jnp.float32))
        (top, numer, denom), unused = lax.scan(step_over, start, (all_keys, all_values, all_pos))
        return (numer / denom[..., None]).astype(jnp.bfloat16)

    result = lax.map(one_block, (all_queries, all_pos))
    return result.reshape(TOKENS, HEADS * HEAD_DIM)
```

```python
import functools
import math

import jax
import jax.numpy as jnp
from jax import lax
from jax.experimental import pallas as pl
from jax.experimental.pallas import tpu as pltpu
from jax.sharding import PartitionSpec as P

HEAD_DIM = 128
NEG_FLOOR = -1e30
MESH = pl.DeviceIdType.MESH
STACK = 4


def attend_kernel(
    n_ctx, n_head, q_ref, k_ref, v_ref, qpos_ref, kpos_ref, out_ref,
    kv, bias, obuf, own_sem, send_sem, recv_sem, osend_sem, orecv_sem, olocal_sem,
):
    rows = q_ref.shape[0]
    kv_local = k_ref.shape[1] // HEAD_DIM
    group = q_ref.shape[1] // HEAD_DIM // kv_local
    subs = group // STACK
    width = STACK * HEAD_DIM
    part = rows // n_head
    chips = n_ctx // 2
    deep = chips // 2
    n_keys = n_ctx * rows

    ctx = lax.axis_index("ctx")
    head = lax.axis_index("head")
    core = lax.rem(ctx, 2)
    chip = ctx // 2
    chip_z, chip_y = chip // 2, lax.rem(chip, 2)
    place = chip_z * (1 - chip_y) + (chips - 1 - chip_z) * chip_y

    def ctx_of(spot, which):
        spot = lax.rem(spot + 2 * chips, chips)
        far = spot // deep
        z = spot * (1 - far) + (chips - 1 - spot) * far
        return (2 * z + far) * 2 + which

    right, left, partner = ctx_of(place + 1, core), ctx_of(place - 1, core), ctx_of(place, 1 - core)

    def own_copies(g):
        cols = pl.ds(g * HEAD_DIM, HEAD_DIM)
        return (
            pltpu.make_async_copy(k_ref.at[:, cols], kv.at[g, ctx, 0], own_sem.at[g, 0]),
            pltpu.make_async_copy(v_ref.at[:, cols], kv.at[g, ctx, 1], own_sem.at[g, 1]),
        )

    for g in range(kv_local):
        for copy in own_copies(g):
            copy.start()

    barrier = pltpu.get_barrier_semaphore()
    for peer in (right, left, partner):
        pl.semaphore_signal(barrier, inc=1, device_id={"ctx": peer}, device_id_type=MESH)
    for hop in range(1, n_head):
        pl.semaphore_signal(
            barrier, inc=1, device_id={"head": lax.rem(head + hop, n_head)}, device_id_type=MESH
        )
    pl.semaphore_wait(barrier, 3 + n_head - 1)

    def ship(g, block, way, number, peer):
        return pltpu.make_async_remote_copy(
            src_ref=kv.at[g, block],
            dst_ref=kv.at[g, block],
            send_sem=send_sem.at[g, way, number],
            recv_sem=recv_sem.at[g, block],
            device_id={"ctx": peer},
            device_id_type=MESH,
        )

    def first_step(g):
        for copy in own_copies(g):
            copy.wait()
        ship(g, ctx, 0, 0, right).start()
        ship(g, ctx, 1, 0, left).start()
        ship(g, ctx, 2, 0, partner).start()

    def right_last(g):
        return deep - lax.rem(g, 2)

    def left_last(g):
        return chips - 1 - right_last(g)

    def later_step(g, step):
        @pl.when(step <= right_last(g))
        def _():
            block = ctx_of(place - step, core)
            ship(g, block, 0, step, right).wait_recv()

            @pl.when(step < right_last(g))
            def _():
                ship(g, block, 0, step, right).start()

            ship(g, block, 2, step, partner).start()

        @pl.when(step <= left_last(g))
        def _():
            block = ctx_of(place + step, core)
            ship(g, block, 1, step, left).wait_recv()

            @pl.when(step < left_last(g))
            def _():
                ship(g, block, 1, step, left).start()

            ship(g, block, 2, chips - step, partner).start()

    def partner_wait(g):
        def one(spot, carry):
            ship(g, ctx_of(spot, 1 - core), 2, 0, partner).wait_recv()
            return carry

        lax.fori_loop(0, chips, one, 0)

    for g in range(kv_local):
        first_step(g)

    bias[...] = jnp.where(kpos_ref[...] <= qpos_ref[...], 0.0, NEG_FLOOR)

    def initial(step, carry):
        later_step(0, step)
        return carry

    lax.fori_loop(1, deep + 1, initial, 0)
    partner_wait(0)

    ring_per_sub = -(-deep // subs)
    factor = HEAD_DIM ** (-0.5) * math.log2(math.e)
    ones = jnp.ones((n_keys, HEAD_DIM), jnp.bfloat16)

    def out_copy(index, peer_head):
        mine = pl.ds(pl.multiple_of((head * kv_local * subs + index) * width, width), width)
        return pltpu.make_async_remote_copy(
            src_ref=obuf.at[peer_head, index],
            dst_ref=out_ref.at[:, mine],
            send_sem=osend_sem.at[peer_head, index],
            recv_sem=orecv_sem.at[head, index],
            device_id={"head": peer_head},
            device_id_type=MESH,
        )

    def in_copy(index, from_head):
        theirs = pl.ds(pl.multiple_of((from_head * kv_local * subs + index) * width, width), width)
        return pltpu.make_async_remote_copy(
            src_ref=obuf.at[head, index],
            dst_ref=out_ref.at[:, theirs],
            send_sem=osend_sem.at[from_head, index],
            recv_sem=orecv_sem.at[from_head, index],
            device_id={"head": from_head},
            device_id_type=MESH,
        )

    def local_copy(index):
        mine = pl.ds(pl.multiple_of((head * kv_local * subs + index) * width, width), width)
        return pltpu.make_async_copy(
            obuf.at[head, index], out_ref.at[:, mine], olocal_sem.at[index]
        )

    def sub_step(index, carry):
        g, sub = index // subs, lax.rem(index, subs)

        @pl.when(g + 1 < kv_local)
        def _():
            for extra in range(ring_per_sub):
                step = sub * ring_per_sub + extra + 1

                @pl.when(step <= deep)
                def _():
                    later_step(g + 1, step)

        @pl.when(jnp.logical_and(g > 0, sub == 0))
        def _():
            partner_wait(g)

        keys = kv[g, :, 0].reshape(n_keys, HEAD_DIM)
        vals = jnp.concatenate([kv[g, :, 1].reshape(n_keys, HEAD_DIM), ones], axis=1)
        start = index * width
        queries = jnp.concatenate(
            [
                q_ref[:, pl.ds(pl.multiple_of(start + j * HEAD_DIM, HEAD_DIM), HEAD_DIM)]
                for j in range(STACK)
            ],
            axis=0,
        )
        scores = lax.dot_general(
            queries, keys, (((1,), (1,)), ((), ())), preferred_element_type=jnp.float32
        )
        scores = (scores.reshape(STACK, rows, n_keys) + bias[...][None]).reshape(STACK * rows, n_keys)
        row_max = jnp.max(scores, axis=1, keepdims=True)
        weights = jnp.exp2((scores - row_max) * factor).astype(jnp.bfloat16)
        both = jnp.dot(weights, vals, preferred_element_type=jnp.float32)
        result = both[:, :HEAD_DIM] / both[:, HEAD_DIM:]
        for j in range(STACK):
            for d in range(n_head):
                piece = result[j * rows + d * part : j * rows + (d + 1) * part]
                obuf[d, index, :, j * HEAD_DIM : (j + 1) * HEAD_DIM] = piece.astype(jnp.bfloat16)
        for hop in range(1, n_head):
            out_copy(index, lax.rem(head + hop, n_head)).start()
        local_copy(index).start()
        return carry

    lax.fori_loop(0, kv_local * subs, sub_step, 0)

    def finish(index, carry):
        for hop in range(1, n_head):
            peer = lax.rem(head + hop, n_head)
            out_copy(index, peer).wait_send()
            in_copy(index, peer).wait_recv()
        local_copy(index).wait()
        return carry

    lax.fori_loop(0, kv_local * subs, finish, 0)

    def drain(g, carry):
        def right_one(step, inner):
            ship(g, ctx, 0, step, right).wait_send()
            return inner

        def left_one(step, inner):
            ship(g, ctx, 1, step, left).wait_send()
            return inner

        def partner_one(step, inner):
            ship(g, ctx, 2, step, partner).wait_send()
            return inner

        lax.fori_loop(0, right_last(g), right_one, 0)
        lax.fori_loop(0, left_last(g), left_one, 0)
        lax.fori_loop(0, chips, partner_one, 0)
        return carry

    lax.fori_loop(0, kv_local, drain, 0)


def per_device(n_ctx, n_head, queries, keys, values, span_pos):
    rows = queries.shape[0]
    span_len = rows // 2
    kv_local = keys.shape[1] // HEAD_DIM
    subs = queries.shape[1] // HEAD_DIM // kv_local // STACK
    chips = n_ctx // 2
    positions = (
        span_pos[:, None] * span_len + jnp.arange(span_len, dtype=jnp.int32)[None, :]
    ).reshape(-1)
    mine = lax.dynamic_slice_in_dim(positions, lax.axis_index("ctx") * rows, rows)
    vmem = pl.BlockSpec(memory_space=pltpu.VMEM)
    n_sub = kv_local * subs
    return pl.pallas_call(
        functools.partial(attend_kernel, n_ctx, n_head),
        out_shape=jax.ShapeDtypeStruct((rows // n_head, queries.shape[1] * n_head), jnp.bfloat16),
        in_specs=[vmem] * 5,
        out_specs=pl.BlockSpec(memory_space=pl.ANY),
        scratch_shapes=[
            pltpu.VMEM((kv_local, n_ctx, 2, rows, HEAD_DIM), jnp.bfloat16),
            pltpu.VMEM((rows, n_ctx * rows), jnp.float32),
            pltpu.VMEM((n_head, n_sub, rows // n_head, STACK * HEAD_DIM), jnp.bfloat16),
            pltpu.SemaphoreType.DMA((kv_local, 2)),
            pltpu.SemaphoreType.DMA((kv_local, 3, chips)),
            pltpu.SemaphoreType.DMA((kv_local, n_ctx)),
            pltpu.SemaphoreType.DMA((n_head, n_sub)),
            pltpu.SemaphoreType.DMA((n_head, n_sub)),
            pltpu.SemaphoreType.DMA((n_sub,)),
        ],
        compiler_params=pltpu.CompilerParams(
            collective_id=0, has_side_effects=True, vmem_limit_bytes=60 * 1024 * 1024
        ),
    )(queries, keys, values, mine[:, None], positions[None, :])


def solution(mesh):
    in_specs = (P("ctx", "head"), P("ctx", "head"), P("ctx", "head"), P())
    out_specs = P(("ctx", "head"), None)
    return jax.shard_map(
        functools.partial(per_device, mesh.shape["ctx"], mesh.shape["head"]),
        mesh=mesh, in_specs=in_specs, out_specs=out_specs, check_vma=False,
    )
```

```python
import functools
import math

import jax
import jax.numpy as jnp
from jax import lax
from jax.experimental import pallas as pl
from jax.experimental.pallas import tpu as pltpu
from jax.sharding import PartitionSpec as P

HEAD_DIM = 128
NEG_FLOOR = -1e30
MESH = pl.DeviceIdType.MESH
STACK = 8
UNIT = 2


def attend_kernel(
    n_ctx, n_head, q_ref, k_ref, v_ref, span_ref, out_ref,
    kv, bias, obuf, own_sem, send_sem, recv_sem, osend_sem, orecv_sem, olocal_sem,
):
    rows = q_ref.shape[0]
    kv_local = k_ref.shape[1] // HEAD_DIM
    group = q_ref.shape[1] // HEAD_DIM // kv_local
    subs = group // STACK
    width = STACK * HEAD_DIM
    part = rows // n_head
    chips = n_ctx // 2
    deep = chips // 2
    n_keys = n_ctx * rows

    ctx = lax.axis_index("ctx")
    head = lax.axis_index("head")
    core = lax.rem(ctx, 2)
    chip = ctx // 2
    chip_z, chip_y = chip // 2, lax.rem(chip, 2)
    place = chip_z * (1 - chip_y) + (chips - 1 - chip_z) * chip_y

    def ctx_of(spot, which):
        spot = lax.rem(spot + 2 * chips, chips)
        far = spot // deep
        z = spot * (1 - far) + (chips - 1 - spot) * far
        return (2 * z + far) * 2 + which

    right, left, partner = ctx_of(place + 1, core), ctx_of(place - 1, core), ctx_of(place, 1 - core)

    def own_copies(g):
        cols = pl.ds(g * HEAD_DIM, HEAD_DIM)
        return (
            pltpu.make_async_copy(k_ref.at[:, cols], kv.at[g, ctx, 0], own_sem.at[g, 0]),
            pltpu.make_async_copy(v_ref.at[:, cols], kv.at[g, ctx, 1], own_sem.at[g, 1]),
        )

    for g in range(kv_local):
        for copy in own_copies(g):
            copy.start()

    barrier = pltpu.get_barrier_semaphore()
    for peer in (right, left, partner):
        pl.semaphore_signal(barrier, inc=1, device_id={"ctx": peer}, device_id_type=MESH)
    for hop in range(1, n_head):
        pl.semaphore_signal(
            barrier, inc=1, device_id={"head": lax.rem(head + hop, n_head)}, device_id_type=MESH
        )
    pl.semaphore_wait(barrier, 3 + n_head - 1)

    def ship(g, block, way, number, peer):
        return pltpu.make_async_remote_copy(
            src_ref=kv.at[g, block],
            dst_ref=kv.at[g, block],
            send_sem=send_sem.at[g, way, number],
            recv_sem=recv_sem.at[g, block],
            device_id={"ctx": peer},
            device_id_type=MESH,
        )

    def first_step(g):
        for copy in own_copies(g):
            copy.wait()
        ship(g, ctx, 0, 0, right).start()
        ship(g, ctx, 1, 0, left).start()
        ship(g, ctx, 2, 0, partner).start()

    def right_last(g):
        return deep - g % 2

    def left_last(g):
        return chips - 1 - right_last(g)

    def later_step(g, step):
        @pl.when(step <= right_last(g))
        def _():
            block = ctx_of(place - step, core)
            ship(g, block, 0, step, right).wait_recv()

            @pl.when(step < right_last(g))
            def _():
                ship(g, block, 0, step, right).start()

            ship(g, block, 2, step, partner).start()

        @pl.when(step <= left_last(g))
        def _():
            block = ctx_of(place + step, core)
            ship(g, block, 1, step, left).wait_recv()

            @pl.when(step < left_last(g))
            def _():
                ship(g, block, 1, step, left).start()

            ship(g, block, 2, chips - step, partner).start()

    def partner_wait(g):
        def one(spot, carry):
            ship(g, ctx_of(spot, 1 - core), 2, 0, partner).wait_recv()
            return carry

        lax.fori_loop(0, chips, one, 0)

    for g in range(kv_local):
        first_step(g)

    span_len = rows // 2
    row = lax.broadcasted_iota(jnp.int32, (rows, 1), 0)
    q_pos = row + jnp.where(
        row < span_len,
        span_ref[2 * ctx] * span_len,
        (span_ref[2 * ctx + 1] - 1) * span_len,
    )
    col = lax.broadcasted_iota(jnp.int32, (1, n_keys), 1)
    k_pos = col
    for span in range(2 * n_ctx):
        k_pos = jnp.where(col >= span * span_len, col + (span_ref[span] - span) * span_len, k_pos)
    bias[...] = jnp.where(k_pos <= q_pos, 0.0, NEG_FLOOR)

    def tick(turn):
        for g in range(kv_local):
            @pl.when(jnp.logical_and(turn - g >= 1, turn - g <= deep))
            def _():
                later_step(g, turn - g)

    def initial(turn, carry):
        tick(turn)
        return carry

    lax.fori_loop(1, deep + 1, initial, 0)

    factor = HEAD_DIM ** (-0.5) * math.log2(math.e)
    ones = jnp.ones((n_keys, HEAD_DIM), jnp.bfloat16)

    def out_copy(index, peer_head):
        mine = pl.ds(pl.multiple_of((head * kv_local * subs + index) * width, width), width)
        return pltpu.make_async_remote_copy(
            src_ref=obuf.at[peer_head, index],
            dst_ref=out_ref.at[:, mine],
            send_sem=osend_sem.at[peer_head, index],
            recv_sem=orecv_sem.at[head, index],
            device_id={"head": peer_head},
            device_id_type=MESH,
        )

    def in_copy(index, from_head):
        theirs = pl.ds(pl.multiple_of((from_head * kv_local * subs + index) * width, width), width)
        return pltpu.make_async_remote_copy(
            src_ref=obuf.at[head, index],
            dst_ref=out_ref.at[:, theirs],
            send_sem=osend_sem.at[from_head, index],
            recv_sem=orecv_sem.at[from_head, index],
            device_id={"head": from_head},
            device_id_type=MESH,
        )

    def local_copy(index):
        mine = pl.ds(pl.multiple_of((head * kv_local * subs + index) * width, width), width)
        return pltpu.make_async_copy(
            obuf.at[head, index], out_ref.at[:, mine], olocal_sem.at[index]
        )

    def sub_step(index, carry):
        g, sub = index // subs, lax.rem(index, subs)

        @pl.when(sub == 0)
        def _():
            partner_wait(g)

        keys = kv[g, :, 0].reshape(n_keys, HEAD_DIM)
        vals = jnp.concatenate([kv[g, :, 1].reshape(n_keys, HEAD_DIM), ones], axis=1)
        start = index * width
        groups = STACK // UNIT

        def make_scores(u):
            queries = jnp.concatenate(
                [
                    q_ref[:, pl.ds(pl.multiple_of(start + (u * UNIT + j) * HEAD_DIM, HEAD_DIM), HEAD_DIM)]
                    for j in range(UNIT)
                ],
                axis=0,
            )
            scores = lax.dot_general(
                queries, keys, (((1,), (1,)), ((), ())), preferred_element_type=jnp.float32
            )
            return (scores.reshape(UNIT, rows, n_keys) + bias[...][None]).reshape(UNIT * rows, n_keys)

        def finish_unit(u, weights):
            both = jnp.dot(weights, vals, preferred_element_type=jnp.float32)
            result = both[:, :HEAD_DIM] / both[:, HEAD_DIM:]
            for j in range(UNIT):
                for d in range(n_head):
                    piece = result[j * rows + d * part : j * rows + (d + 1) * part]
                    at = (u * UNIT + j) * HEAD_DIM
                    obuf[d, index, :, at : at + HEAD_DIM] = piece.astype(jnp.bfloat16)

        scores = make_scores(0)
        for u in range(groups):
            following = make_scores(u + 1) if u + 1 < groups else None
            row_max = jnp.max(scores, axis=1, keepdims=True)
            weights = jnp.exp2((scores - row_max) * factor).astype(jnp.bfloat16)
            finish_unit(u, weights)
            scores = following
        for hop in range(1, n_head):
            out_copy(index, lax.rem(head + hop, n_head)).start()
        local_copy(index).start()

        @pl.when(index + 1 < kv_local)
        def _():
            tick(deep + 1 + index)

        return carry

    lax.fori_loop(0, kv_local * subs, sub_step, 0)

    def finish(index, carry):
        for hop in range(1, n_head):
            peer = lax.rem(head + hop, n_head)
            out_copy(index, peer).wait_send()
            in_copy(index, peer).wait_recv()
        local_copy(index).wait()
        return carry

    lax.fori_loop(0, kv_local * subs, finish, 0)

    def drain(g, carry):
        def right_one(step, inner):
            ship(g, ctx, 0, step, right).wait_send()
            return inner

        def left_one(step, inner):
            ship(g, ctx, 1, step, left).wait_send()
            return inner

        def partner_one(step, inner):
            ship(g, ctx, 2, step, partner).wait_send()
            return inner

        lax.fori_loop(0, right_last(g), right_one, 0)
        lax.fori_loop(0, left_last(g), left_one, 0)
        lax.fori_loop(0, chips, partner_one, 0)
        return carry

    lax.fori_loop(0, kv_local, drain, 0)


def per_device(n_ctx, n_head, queries, keys, values, span_pos):
    rows = queries.shape[0]
    kv_local = keys.shape[1] // HEAD_DIM
    subs = queries.shape[1] // HEAD_DIM // kv_local // STACK
    chips = n_ctx // 2
    vmem = pl.BlockSpec(memory_space=pltpu.VMEM)
    n_sub = kv_local * subs
    return pl.pallas_call(
        functools.partial(attend_kernel, n_ctx, n_head),
        out_shape=jax.ShapeDtypeStruct((rows // n_head, queries.shape[1] * n_head), jnp.bfloat16),
        in_specs=[vmem] * 3 + [pl.BlockSpec(memory_space=pltpu.SMEM)],
        out_specs=pl.BlockSpec(memory_space=pl.ANY),
        scratch_shapes=[
            pltpu.VMEM((kv_local, n_ctx, 2, rows, HEAD_DIM), jnp.bfloat16),
            pltpu.VMEM((rows, n_ctx * rows), jnp.float32),
            pltpu.VMEM((n_head, n_sub, rows // n_head, STACK * HEAD_DIM), jnp.bfloat16),
            pltpu.SemaphoreType.DMA((kv_local, 2)),
            pltpu.SemaphoreType.DMA((kv_local, 3, chips)),
            pltpu.SemaphoreType.DMA((kv_local, n_ctx)),
            pltpu.SemaphoreType.DMA((n_head, n_sub)),
            pltpu.SemaphoreType.DMA((n_head, n_sub)),
            pltpu.SemaphoreType.DMA((n_sub,)),
        ],
        compiler_params=pltpu.CompilerParams(
            collective_id=0, has_side_effects=True, vmem_limit_bytes=60 * 1024 * 1024
        ),
    )(queries, keys, values, span_pos)


def solution(mesh):
    in_specs = (P("ctx", "head"), P("ctx", "head"), P("ctx", "head"), P())
    out_specs = P(("ctx", "head"), None)
    return jax.shard_map(
        functools.partial(per_device, mesh.shape["ctx"], mesh.shape["head"]),
        mesh=mesh, in_specs=in_specs, out_specs=out_specs, check_vma=False,
    )
```

```python
import functools
import math

import jax
import jax.numpy as jnp
from jax import lax
from jax.experimental import pallas as pl
from jax.experimental.pallas import tpu as pltpu
from jax.sharding import PartitionSpec as P

HEAD_DIM = 128
NEG_FLOOR = -1e30
MESH = pl.DeviceIdType.MESH
STACK = 16
UNIT = 2


def attend_kernel(
    n_ctx, n_head, q_ref, k_ref, v_ref, span_ref, out_ref,
    kv, bias, obuf, own_sem, send_sem, recv_sem, osend_sem, orecv_sem, olocal_sem,
):
    rows = q_ref.shape[0]
    kv_local = k_ref.shape[1] // HEAD_DIM
    group = q_ref.shape[1] // HEAD_DIM // kv_local
    subs = group // STACK
    width = STACK * HEAD_DIM
    part = rows // n_head
    chips = n_ctx // 2
    deep = chips // 2
    n_keys = n_ctx * rows

    ctx = lax.axis_index("ctx")
    head = lax.axis_index("head")
    core = lax.rem(ctx, 2)
    chip = ctx // 2
    chip_z, chip_y = chip // 2, lax.rem(chip, 2)
    place = chip_z * (1 - chip_y) + (chips - 1 - chip_z) * chip_y

    def ctx_of(spot, which):
        spot = lax.rem(spot + 2 * chips, chips)
        far = spot // deep
        z = spot * (1 - far) + (chips - 1 - spot) * far
        return (2 * z + far) * 2 + which

    right, left, partner = ctx_of(place + 1, core), ctx_of(place - 1, core), ctx_of(place, 1 - core)

    def own_copies(g):
        cols = pl.ds(g * HEAD_DIM, HEAD_DIM)
        return (
            pltpu.make_async_copy(k_ref.at[:, cols], kv.at[g, ctx, 0], own_sem.at[g, 0]),
            pltpu.make_async_copy(v_ref.at[:, cols], kv.at[g, ctx, 1], own_sem.at[g, 1]),
        )

    for g in range(kv_local):
        for copy in own_copies(g):
            copy.start()

    barrier = pltpu.get_barrier_semaphore()
    for peer in (right, left, partner):
        pl.semaphore_signal(barrier, inc=1, device_id={"ctx": peer}, device_id_type=MESH)
    for hop in range(1, n_head):
        pl.semaphore_signal(
            barrier, inc=1, device_id={"head": lax.rem(head + hop, n_head)}, device_id_type=MESH
        )
    pl.semaphore_wait(barrier, 3 + n_head - 1)

    def ship(g, block, way, number, peer):
        return pltpu.make_async_remote_copy(
            src_ref=kv.at[g, block],
            dst_ref=kv.at[g, block],
            send_sem=send_sem.at[g, way, number],
            recv_sem=recv_sem.at[g, block],
            device_id={"ctx": peer},
            device_id_type=MESH,
        )

    def first_step(g):
        for copy in own_copies(g):
            copy.wait()
        ship(g, ctx, 0, 0, right).start()
        ship(g, ctx, 1, 0, left).start()
        ship(g, ctx, 2, 0, partner).start()

    def right_last(g):
        return deep - g % 2

    def left_last(g):
        return chips - 1 - right_last(g)

    def later_step(g, step):
        @pl.when(step <= right_last(g))
        def _():
            block = ctx_of(place - step, core)
            ship(g, block, 0, step, right).wait_recv()

            @pl.when(step < right_last(g))
            def _():
                ship(g, block, 0, step, right).start()

            ship(g, block, 2, step, partner).start()

        @pl.when(step <= left_last(g))
        def _():
            block = ctx_of(place + step, core)
            ship(g, block, 1, step, left).wait_recv()

            @pl.when(step < left_last(g))
            def _():
                ship(g, block, 1, step, left).start()

            ship(g, block, 2, chips - step, partner).start()

    def partner_wait(g):
        def one(spot, carry):
            ship(g, ctx_of(spot, 1 - core), 2, 0, partner).wait_recv()
            return carry

        lax.fori_loop(0, chips, one, 0)

    for g in range(kv_local):
        first_step(g)

    span_len = rows // 2
    row = lax.broadcasted_iota(jnp.int32, (rows, 1), 0)
    q_pos = row + jnp.where(
        row < span_len,
        span_ref[2 * ctx] * span_len,
        (span_ref[2 * ctx + 1] - 1) * span_len,
    )
    col = lax.broadcasted_iota(jnp.int32, (1, n_keys), 1)
    k_pos = col
    for span in range(2 * n_ctx):
        k_pos = jnp.where(col >= span * span_len, col + (span_ref[span] - span) * span_len, k_pos)
    bias[...] = jnp.where(k_pos <= q_pos, 0.0, NEG_FLOOR)

    def tick(turn):
        for g in range(kv_local):
            @pl.when(jnp.logical_and(turn - g >= 1, turn - g <= deep))
            def _():
                later_step(g, turn - g)

    def initial(turn, carry):
        tick(turn)
        return carry

    lax.fori_loop(1, deep + 1, initial, 0)

    factor = HEAD_DIM ** (-0.5) * math.log2(math.e)
    ones = jnp.ones((n_keys, HEAD_DIM), jnp.bfloat16)

    def out_copy(index, peer_head):
        mine = pl.ds(pl.multiple_of((head * kv_local * subs + index) * width, width), width)
        return pltpu.make_async_remote_copy(
            src_ref=obuf.at[peer_head, index],
            dst_ref=out_ref.at[:, mine],
            send_sem=osend_sem.at[peer_head, index],
            recv_sem=orecv_sem.at[head, index],
            device_id={"head": peer_head},
            device_id_type=MESH,
        )

    def in_copy(index, from_head):
        theirs = pl.ds(pl.multiple_of((from_head * kv_local * subs + index) * width, width), width)
        return pltpu.make_async_remote_copy(
            src_ref=obuf.at[head, index],
            dst_ref=out_ref.at[:, theirs],
            send_sem=osend_sem.at[from_head, index],
            recv_sem=orecv_sem.at[from_head, index],
            device_id={"head": from_head},
            device_id_type=MESH,
        )

    def local_copy(index):
        mine = pl.ds(pl.multiple_of((head * kv_local * subs + index) * width, width), width)
        return pltpu.make_async_copy(
            obuf.at[head, index], out_ref.at[:, mine], olocal_sem.at[index]
        )

    def sub_step(index, carry):
        g, sub = index // subs, lax.rem(index, subs)

        @pl.when(sub == 0)
        def _():
            partner_wait(g)

        keys = kv[g, :, 0].reshape(n_keys, HEAD_DIM)
        vals = jnp.concatenate([kv[g, :, 1].reshape(n_keys, HEAD_DIM), ones], axis=1)
        start = index * width
        groups = STACK // UNIT

        def make_scores(u):
            queries = jnp.concatenate(
                [
                    q_ref[:, pl.ds(pl.multiple_of(start + (u * UNIT + j) * HEAD_DIM, HEAD_DIM), HEAD_DIM)]
                    for j in range(UNIT)
                ],
                axis=0,
            )
            scores = lax.dot_general(
                queries, keys, (((1,), (1,)), ((), ())), preferred_element_type=jnp.float32
            )
            return (scores.reshape(UNIT, rows, n_keys) + bias[...][None]).reshape(UNIT * rows, n_keys)

        def finish_unit(u, weights):
            both = jnp.dot(weights, vals, preferred_element_type=jnp.float32)
            result = both[:, :HEAD_DIM] / both[:, HEAD_DIM:]
            for j in range(UNIT):
                for d in range(n_head):
                    piece = result[j * rows + d * part : j * rows + (d + 1) * part]
                    at = (u * UNIT + j) * HEAD_DIM
                    obuf[d, index, :, at : at + HEAD_DIM] = piece.astype(jnp.bfloat16)

        scores = make_scores(0)
        for u in range(groups):
            following = make_scores(u + 1) if u + 1 < groups else None
            row_max = jnp.max(scores, axis=1, keepdims=True)
            weights = jnp.exp2((scores - row_max) * factor).astype(jnp.bfloat16)
            finish_unit(u, weights)
            scores = following
        for hop in range(1, n_head):
            out_copy(index, lax.rem(head + hop, n_head)).start()
        local_copy(index).start()

        @pl.when(index + 1 < kv_local)
        def _():
            tick(deep + 1 + index)

        return carry

    lax.fori_loop(0, kv_local * subs, sub_step, 0)

    def finish(index, carry):
        for hop in range(1, n_head):
            peer = lax.rem(head + hop, n_head)
            out_copy(index, peer).wait_send()
            in_copy(index, peer).wait_recv()
        local_copy(index).wait()
        return carry

    lax.fori_loop(0, kv_local * subs, finish, 0)

    def drain(g, carry):
        def right_one(step, inner):
            ship(g, ctx, 0, step, right).wait_send()
            return inner

        def left_one(step, inner):
            ship(g, ctx, 1, step, left).wait_send()
            return inner

        def partner_one(step, inner):
            ship(g, ctx, 2, step, partner).wait_send()
            return inner

        lax.fori_loop(0, right_last(g), right_one, 0)
        lax.fori_loop(0, left_last(g), left_one, 0)
        lax.fori_loop(0, chips, partner_one, 0)
        return carry

    lax.fori_loop(0, kv_local, drain, 0)


def per_device(n_ctx, n_head, queries, keys, values, span_pos):
    rows = queries.shape[0]
    kv_local = keys.shape[1] // HEAD_DIM
    subs = queries.shape[1] // HEAD_DIM // kv_local // STACK
    chips = n_ctx // 2
    vmem = pl.BlockSpec(memory_space=pltpu.VMEM)
    n_sub = kv_local * subs
    return pl.pallas_call(
        functools.partial(attend_kernel, n_ctx, n_head),
        out_shape=jax.ShapeDtypeStruct((rows // n_head, queries.shape[1] * n_head), jnp.bfloat16),
        in_specs=[vmem] * 3 + [pl.BlockSpec(memory_space=pltpu.SMEM)],
        out_specs=pl.BlockSpec(memory_space=pl.ANY),
        scratch_shapes=[
            pltpu.VMEM((kv_local, n_ctx, 2, rows, HEAD_DIM), jnp.bfloat16),
            pltpu.VMEM((rows, n_ctx * rows), jnp.float32),
            pltpu.VMEM((n_head, n_sub, rows // n_head, STACK * HEAD_DIM), jnp.bfloat16),
            pltpu.SemaphoreType.DMA((kv_local, 2)),
            pltpu.SemaphoreType.DMA((kv_local, 3, chips)),
            pltpu.SemaphoreType.DMA((kv_local, n_ctx)),
            pltpu.SemaphoreType.DMA((n_head, n_sub)),
            pltpu.SemaphoreType.DMA((n_head, n_sub)),
            pltpu.SemaphoreType.DMA((n_sub,)),
        ],
        compiler_params=pltpu.CompilerParams(
            collective_id=0, has_side_effects=True, vmem_limit_bytes=60 * 1024 * 1024
        ),
    )(queries, keys, values, span_pos)


def solution(mesh):
    in_specs = (P("ctx", "head"), P("ctx", "head"), P("ctx", "head"), P())
    out_specs = P(("ctx", "head"), None)
    return jax.shard_map(
        functools.partial(per_device, mesh.shape["ctx"], mesh.shape["head"]),
        mesh=mesh, in_specs=in_specs, out_specs=out_specs, check_vma=False,
    )
```
